32 devices in a mesh: rep: 2 (over y), dev: 4 (over z), col: 4 (over x, core).
Axes of the slice: x: 2, y: 2, z: 4, core: 2. Of those that a mesh axis runs over, the one named last changes fastest.
Arguments:
- queries: bfloat16 [256, 8192], P(('rep', 'dev'), 'col'), parts along dimension 0
- kv_pages: bfloat16 [768, 8, 2, 128, 128], P(('rep', 'dev'), 'col'), parts along dimension 0
- page_table: int32 [256, 3], P(('rep', 'dev')), parts along dimension 0, may hold values from 0 to 95, as said below
- seq_lengths: int32 [256], P(('rep', 'dev')), parts along dimension 0, may hold values from 2 to 384, as said below
- ffn_seat: int32 [256], P('rep'), parts along dimension 0, may hold values from 0 to 127, each once
- resid: bfloat16 [256, 8192], P(('rep', 'col'), 'dev'), parts along dimension 0, may hold values from -6 to 6
- w_out: bfloat16 [8192, 8192], P('col', 'dev'), may hold values from -0.0625 to 0.0625
- norm_gain: float32 [8192], P('dev'), may hold values from 0.25 to 1.75
- w_gate: bfloat16 [8192, 14336], P('dev', 'col'), may hold values from -0.0625 to 0.0625
- w_up: bfloat16 [8192, 14336], P('dev', 'col'), may hold values from -0.0625 to 0.0625
- w_down: bfloat16 [14336, 8192], P('col', 'dev'), may hold values from -0.046875 to 0.046875
Outputs:
- layer_out: bfloat16 [256, 8192], P(('rep', 'col'), 'dev'), parts along dimension 0
The draws below stay inside these ranges and needn't reach their ends.
There are 2 independent parts, one for each index of `rep`. The reference program is written for one: setup_inputs(seed, part) draws one part's arguments, and reference() takes and returns one part's arrays. A program takes and returns all parts, laid end to end along the dimension named above; an argument that names none is the same for every part. Nothing has to cross between parts.
Inputs may be any that keep to these rules, and one draw needn't show every extreme that they name: `page_table`: the 32 rows of one dev index hold each block 0 to 95 of that index's pool exactly once. `seq_lengths`: the first sequence has 384 cached tokens.
All inputs are finite; a program needn't handle non-finite values.
Results may differ from the reference program's by a relative error of at most 0.017.
Values may be sent and summed in bfloat16 or wider, within the bound.
A program may use at most 128 MiB of HBM per device.

```python
import jax
import jax.numpy as jnp
from jax import lax

HQ = 64
KVH = 8
HD = 128
D = 8192
FF = 14336
SEQ_DEV = 32
PAGE = 128
MAXP = 3
POOL = 96
MAXLEN = 384
TOKENS = 128
N_DEV = 4


def layout_ints(key):
    base = jax.random.fold_in(key, 101)
    first_key, second_key, third_key = jax.random.split(base, 3)
    ceilings = jax.random.randint(first_key, (N_DEV, 1), MAXLEN // 4, MAXLEN + 1)
    raw_bits = jax.random.randint(second_key, (N_DEV, SEQ_DEV), 0, 1 << 30)
    lengths = 2 + raw_bits % (ceilings - 1)
    lengths = lengths.reshape(-1).at[0].set(MAXLEN)
    group_keys = jax.random.split(third_key, N_DEV)
    tables = jax.vmap(lambda one_key: jax.random.permutation(one_key, POOL))(group_keys)
    return (lengths.astype(jnp.int32), tables.reshape(SEQ_DEV * N_DEV, MAXP).astype(jnp.int32))


def draw_seq_lengths(key, part):
    return layout_ints(key)[0]


def draw_page_table(key, part):
    return layout_ints(key)[1]


def draw_kv_pages(key, part):
    values = jnp.clip(jax.random.normal(jax.random.fold_in(key, 202), (N_DEV * POOL, KVH, 2, PAGE, HD), jnp.float32), -5.0, 5.0)
    return values.astype(jnp.bfloat16)


def draw_queries(key, part):
    tokens = SEQ_DEV * N_DEV
    query = jnp.clip(jax.random.normal(jax.random.fold_in(key, 301), (tokens, HQ, HD), jnp.float32), -5.0, 5.0)
    return query.reshape(tokens, HQ * HD).astype(jnp.bfloat16)


def block_levels(key, dims, cuts, smallest, largest):
    level, own = 1.0, jax.random.fold_in(key, 6)
    for position, blocks in cuts:
        steps = jnp.exp(jax.random.uniform(jax.random.fold_in(own, position), (blocks,), jnp.float32, smallest / len(cuts), largest / len(cuts)))
        level = level * jnp.repeat(steps, dims[position] // blocks).reshape([-1 if axis == position else 1 for axis in range(len(dims))])
    return level


def scatter_about(stream_key, extent, spread, bound, cuts=(), kind=jnp.bfloat16):
    array = spread * jax.random.normal(stream_key, extent, jnp.float32)
    if cuts:
        array = array * block_levels(stream_key, extent, cuts, -0.22, 0.18)
    return jnp.clip(array, -bound, bound).astype(kind)


def setup_inputs(seed: int = 0, part: int = 0) -> dict:
    seeds = jax.random.split(jax.random.key(seed), 12)
    part_splits = jax.random.split(jax.random.fold_in(seeds[11], part), 12)
    return {
        "queries": draw_queries(jax.random.fold_in(jax.random.fold_in(seeds[11], part), 71), part),
        "kv_pages": draw_kv_pages(jax.random.fold_in(jax.random.fold_in(seeds[11], part), 71), part),
        "page_table": draw_page_table(jax.random.fold_in(jax.random.fold_in(seeds[11], part), 71), part),
        "seq_lengths": draw_seq_lengths(jax.random.fold_in(jax.random.fold_in(seeds[11], part), 71), part),
        "ffn_seat": jax.random.permutation(part_splits[4], TOKENS).astype(jnp.int32),
        "resid": scatter_about(part_splits[5], (TOKENS, D), 1.0, 6.0, ((0, 4), (1, 4))),
        "w_out": scatter_about(seeds[6], (D, D), D ** -0.5, 0.0625, ((0, 4), (1, 4))),
        "norm_gain": jnp.clip(1.0 + 0.15 * jax.random.normal(seeds[7], (D,), jnp.float32), 0.25, 1.75),
        "w_gate": scatter_about(seeds[8], (D, FF), D ** -0.5, 0.0625, ((0, 4), (1, 4))),
        "w_up": scatter_about(seeds[9], (D, FF), D ** -0.5, 0.0625, ((0, 4), (1, 4))),
        "w_down": scatter_about(seeds[10], (FF, D), FF ** -0.5, 0.046875, ((0, 4), (1, 4))),
    }


def attend_group(operands):
    query, kv_group, table, lengths = operands
    group_size = HQ // KVH
    kv_blocks = kv_group[table]
    key_span = MAXP * PAGE
    key_rows = kv_blocks[:, :, :, 0].transpose(0, 2, 1, 3, 4).reshape(SEQ_DEV, KVH, key_span, HD)
    value_rows = kv_blocks[:, :, :, 1].transpose(0, 2, 1, 3, 4).reshape(SEQ_DEV, KVH, key_span, HD)
    query_heads = query.reshape(SEQ_DEV, KVH, group_size, HD)
    scores = jnp.einsum('skgd,sktd->skgt', query_heads.astype(jnp.float32), key_rows.astype(jnp.float32)) * HD ** (-0.5)
    live_mask = jnp.arange(key_span)[None, :] < lengths[:, None]
    scores = jnp.where(live_mask[:, None, None, :], scores, -1e+30)
    top = lax.optimization_barrier(jnp.max(scores, axis=-1, keepdims=True))
    expo = jnp.exp(scores - top)
    weights = (expo / lax.optimization_barrier(jnp.sum(expo, axis=-1, keepdims=True))).astype(jnp.bfloat16)
    attended = jnp.einsum('skgt,sktd->skgd', weights.astype(jnp.float32), value_rows.astype(jnp.float32))
    return attended.astype(jnp.bfloat16).reshape(SEQ_DEV, HQ * HD)

def reference(queries, kv_pages, page_table, seq_lengths, ffn_seat, resid, w_out, norm_gain, w_gate, w_up, w_down):
    width = HQ * HD
    attended = lax.map(attend_group, (queries.reshape(N_DEV, SEQ_DEV, width), kv_pages.reshape(N_DEV, POOL, KVH, 2, PAGE, HD), page_table.reshape(N_DEV, SEQ_DEV, MAXP), seq_lengths.reshape(N_DEV, SEQ_DEV)))
    attended = attended.reshape(SEQ_DEV * N_DEV, width)
    projected = jnp.dot(attended, w_out, preferred_element_type=jnp.float32)
    placed = jnp.zeros_like(projected).at[ffn_seat].set(projected)
    stream = resid.astype(jnp.float32) + placed
    mean_sq = lax.optimization_barrier(jnp.mean(stream * stream, axis=1))
    normed = (stream * lax.rsqrt(mean_sq + 1e-05)[:, None] * norm_gain[None, :]).astype(jnp.bfloat16)
    gate = jnp.dot(normed, w_gate, preferred_element_type=jnp.float32)
    up_part = jnp.dot(normed, w_up, preferred_element_type=jnp.float32)
    hidden = (jax.nn.silu(gate) * up_part).astype(jnp.bfloat16)
    ffn_out = jnp.dot(hidden, w_down, preferred_element_type=jnp.float32)
    return (stream + ffn_out).astype(jnp.bfloat16)
```

```python
import functools

import jax
import jax.numpy as jnp
from jax import lax
from jax.experimental import pallas as pl
from jax.experimental.pallas import tpu as pltpu
from jax.sharding import PartitionSpec as P

MESH = pl.DeviceIdType.MESH
F32 = jnp.float32
BF16 = jnp.bfloat16


def divisor(size, choices):
    for choice in choices:
        if size % choice == 0:
            return choice
    return size


def attend_kernel(seqs, pages, kv_local, table_ref, len_ref, q_ref, *refs):
    blocks, out_ref = refs[:-1], refs[-1]
    step = pl.program_id(0)
    page, head_dim = blocks[0].shape[3], blocks[0].shape[4]
    span = pages * page
    scale = head_dim ** (-0.5)
    for s in range(seqs):
        length = len_ref[step * seqs + s]
        for h in range(kv_local):
            query = q_ref[s, h]
            scores = jnp.concatenate(
                [
                    lax.dot_general(
                        query,
                        blocks[s * pages + j][0, h, 0],
                        (((1,), (1,)), ((), ())),
                        preferred_element_type=F32,
                    )
                    for j in range(pages)
                ],
                axis=1,
            ) * scale
            live = lax.broadcasted_iota(jnp.int32, scores.shape, 1) < length
            scores = jnp.where(live, scores, -1e30)
            top = jnp.max(scores, axis=1, keepdims=True)
            expo = jnp.exp(scores - top)
            weights = (expo / jnp.sum(expo, axis=1, keepdims=True)).astype(BF16)
            total = None
            for j in range(pages):
                part = jnp.dot(
                    weights[:, j * page : (j + 1) * page],
                    blocks[s * pages + j][0, h, 1],
                    preferred_element_type=F32,
                )
                total = part if total is None else total + part
            out_ref[s, h] = total.astype(BF16)


def attend(queries, kv_pages, page_table, seq_lengths):
    count = queries.shape[0]
    _, kv_local, _, page, head_dim = kv_pages.shape
    pages = page_table.shape[1]
    group = queries.shape[1] // (kv_local * head_dim)
    seqs = divisor(count, (4, 2, 1))

    def block_map(s, j, i, table, lens):
        return (table[(i * seqs + s) * pages + j], 0, 0, 0, 0)

    kv_specs = [
        pl.BlockSpec((1, kv_local, 2, page, head_dim), functools.partial(block_map, s, j))
        for s in range(seqs)
        for j in range(pages)
    ]
    q_spec = pl.BlockSpec((seqs, kv_local, group, head_dim), lambda i, table, lens: (i, 0, 0, 0))
    out = pl.pallas_call(
        functools.partial(attend_kernel, seqs, pages, kv_local),
        grid_spec=pltpu.PrefetchScalarGridSpec(
            num_scalar_prefetch=2,
            grid=(count // seqs,),
            in_specs=[q_spec] + kv_specs,
            out_specs=q_spec,
        ),
        out_shape=jax.ShapeDtypeStruct((count, kv_local, group, head_dim), BF16),
        compiler_params=pltpu.CompilerParams(dimension_semantics=("arbitrary",)),
    )(
        page_table.reshape(-1),
        seq_lengths,
        queries.reshape(count, kv_local, group, head_dim),
        *([kv_pages] * len(kv_specs)),
    )
    return out.reshape(count, -1)


def layer_kernel(
    nd,
    nc,
    dims,
    att_ref,
    seat_ref,
    resid_ref,
    gain_ref,
    wo_hbm,
    wg_hbm,
    wu_hbm,
    wd_hbm,
    out_ref,
    wo,
    wg,
    wu,
    wd,
    att_all,
    seated,
    proj,
    rs_in,
    x_all,
    ss_all,
    stream,
    own,
    in_r,
    in_l,
    ss_own,
    ss_r,
    ss_l,
    inv,
    hid,
    acc,
    down,
    down_in,
    w_sem,
    f_sem,
    att_s,
    att_r,
    rs_s,
    rs_r,
    x_s,
    x_r,
    ssc_s,
    ssc_r,
    sum_s,
    sum_r,
    ssd_s,
    ssd_r,
    hid_s,
    hid_r,
    dn_s,
    dn_r,
):
    T, B, R, HK, WC, NJ, AC, NA, CF, NC, half, full = dims
    me = lax.axis_index("dev")
    mc = lax.axis_index("col")
    E = nd - 1

    def peer_of(k):
        return lax.rem(mc + k, nc)

    def wo_copy(j):
        cols = pl.ds(pl.multiple_of(j * WC, WC), WC)
        return pltpu.make_async_copy(wo_hbm.at[:, cols], wo.at[j], w_sem.at[j])

    def ffn_copy(which, c):
        span = pl.ds(pl.multiple_of(c * CF, CF), CF)
        source = (wg_hbm.at[:, span], wu_hbm.at[:, span], wd_hbm.at[span, :])[which]
        return pltpu.make_async_copy(source, (wg, wu, wd)[which].at[c], f_sem.at[which, c])

    @pl.loop(0, NJ)
    def _(j):
        wo_copy(j).start()

    @pl.loop(0, NC)
    def _(c):
        ffn_copy(0, c).start()
        ffn_copy(1, c).start()

    @pl.loop(0, NC)
    def _(c):
        ffn_copy(2, c).start()

    barrier = pltpu.get_barrier_semaphore()

    @pl.when(me > 0)
    def _():
        pl.semaphore_signal(barrier, inc=1, device_id={"dev": me - 1}, device_id_type=MESH)

    @pl.when(me < E)
    def _():
        pl.semaphore_signal(barrier, inc=1, device_id={"dev": me + 1}, device_id_type=MESH)

    for k in range(1, nc):
        pl.semaphore_signal(barrier, inc=1, device_id={"col": peer_of(k)}, device_id_type=MESH)

    neighbours = jnp.where(me > 0, 1, 0) + jnp.where(me < E, 1, 0)
    pl.semaphore_wait(barrier, neighbours + (nc - 1))

    def att_rows(origin):
        return pl.ds(pl.multiple_of(origin * B, B), B)

    def att_copy(origin, a, way, from_input):
        cols = slice(a * AC, (a + 1) * AC)
        dst = att_all.at[att_rows(origin), cols]
        return pltpu.make_async_remote_copy(
            src_ref=att_ref.at[:, cols] if from_input else dst,
            dst_ref=dst,
            send_sem=att_s.at[way, origin, a],
            recv_sem=att_r.at[origin, a],
            device_id={"dev": me + (1 if way == 0 else -1)},
            device_id_type=MESH,
        )

    for a in range(NA):
        @pl.when(me < E)
        def _():
            att_copy(me, a, 0, True).start()

        @pl.when(me > 0)
        def _():
            att_copy(me, a, 1, True).start()

    att_all[att_rows(me), :] = att_ref[...]

    @pl.loop(1, nd)
    def _(k):
        for a in range(NA):
            @pl.when(me - k >= 0)
            def _():
                att_copy(me - k, a, 0, False).wait_recv()

                @pl.when(me < E)
                def _():
                    att_copy(me - k, a, 0, False).start()

            @pl.when(me + k <= E)
            def _():
                att_copy(me + k, a, 1, False).wait_recv()

                @pl.when(me > 0)
                def _():
                    att_copy(me + k, a, 1, False).start()

    pick = (lax.broadcasted_iota(jnp.int32, (T, T), 0) == seat_ref[...]).astype(F32).astype(BF16)
    seated[...] = jnp.dot(pick, att_all[...], preferred_element_type=F32).astype(BF16)

    def rs_copy(k, j, source, target, send, recv):
        cols = pl.ds(pl.multiple_of(j * WC, WC), WC)
        rows = pl.ds(pl.multiple_of(peer_of(k) * R, R), R)
        return pltpu.make_async_remote_copy(
            src_ref=source.at[rows, cols],
            dst_ref=target.at[k - 1, :, cols],
            send_sem=send.at[k - 1, j],
            recv_sem=recv.at[k - 1, j],
            device_id={"col": peer_of(k)},
            device_id_type=MESH,
        )

    @pl.loop(0, NJ)
    def _(j):
        wo_copy(j).wait()
        cols = pl.ds(pl.multiple_of(j * WC, WC), WC)
        proj[:, cols] = jnp.dot(seated[...], wo[j], preferred_element_type=F32).astype(BF16)
        for k in range(1, nc):
            rs_copy(k, j, proj, rs_in, rs_s, rs_r).start()

    my_rows = pl.ds(pl.multiple_of(mc * R, R), R)

    def x_copy(k, j):
        spot = x_all.at[my_rows, pl.ds(pl.multiple_of(j * WC, WC), WC)]
        return pltpu.make_async_remote_copy(
            src_ref=spot,
            dst_ref=spot,
            send_sem=x_s.at[k - 1, j],
            recv_sem=x_r.at[k - 1, j],
            device_id={"col": peer_of(k)},
            device_id_type=MESH,
        )

    def ssc_copy(k):
        spot = ss_all.at[my_rows, :]
        return pltpu.make_async_remote_copy(
            src_ref=spot,
            dst_ref=spot,
            send_sem=ssc_s.at[k - 1],
            recv_sem=ssc_r.at[k - 1],
            device_id={"col": peer_of(k)},
            device_id_type=MESH,
        )

    squares = jnp.zeros((R, 1), F32)
    for j in range(NJ):
        cols = slice(j * WC, (j + 1) * WC)
        value = resid_ref[:, cols].astype(F32) + proj[my_rows, cols].astype(F32)
        for k in range(1, nc):
            rs_copy(k, j, proj, rs_in, rs_s, rs_r).wait_recv()
            value = value + rs_in[k - 1, :, cols].astype(F32)
        stream[:, cols] = value
        squares = squares + jnp.sum(value * value, axis=1, keepdims=True)
        x_all[my_rows, cols] = (value * gain_ref[:, cols]).astype(BF16)
        for k in range(1, nc):
            x_copy(k, j).start()
    ss_all[my_rows, :] = jnp.broadcast_to(squares, (R, ss_all.shape[1]))
    for k in range(1, nc):
        ssc_copy(k).start()
    for k in range(1, nc):
        for j in range(NJ):
            x_copy(k, j).wait_recv()
        ssc_copy(k).wait_recv()
    ss_own[...] = ss_all[...]

    def neighbour(way):
        return {"dev": me + (1 if way == 0 else -1)}

    def sum_copy(way, c):
        return pltpu.make_async_remote_copy(
            src_ref=own.at[c, 1 - way],
            dst_ref=(in_r if way == 0 else in_l).at[c],
            send_sem=sum_s.at[way, c],
            recv_sem=sum_r.at[way, c],
            device_id=neighbour(way),
            device_id_type=MESH,
        )

    def ssd_copy(way):
        return pltpu.make_async_remote_copy(
            src_ref=ss_own.at[pl.ds((1 - way) * half, half), :],
            dst_ref=ss_r if way == 0 else ss_l,
            send_sem=ssd_s.at[way],
            recv_sem=ssd_r.at[way],
            device_id=neighbour(way),
            device_id_type=MESH,
        )

    def hid_copy(way, c):
        spot = hid.at[c, pl.ds(way * half, half), :]
        return pltpu.make_async_remote_copy(
            src_ref=spot,
            dst_ref=spot,
            send_sem=hid_s.at[way, c],
            recv_sem=hid_r.at[way, c],
            device_id=neighbour(way),
            device_id_type=MESH,
        )

    def sum_stage(way, c):
        first = 0 if way == 0 else E
        last = E - first
        part = 1 - way
        incoming = in_r if way == 0 else in_l
        ss_in = ss_r if way == 0 else ss_l
        ss_rows = pl.ds(part * half, half)

        @pl.when(c == 0)
        def _():
            @pl.when(me != first)
            def _():
                ssd_copy(way).wait_recv()
                ss_own[ss_rows, :] = ss_own[ss_rows, :] + ss_in[...]

            @pl.when(me != last)
            def _():
                ssd_copy(way).start()

            @pl.when(me == last)
            def _():
                inv[...] = lax.rsqrt(ss_own[ss_rows, :] / full + 1e-5)

        @pl.when(me != first)
        def _():
            sum_copy(way, c).wait_recv()

            @pl.when(me != last)
            def _():
                total = own[c, part].astype(F32) + incoming[c].astype(F32)
                own[c, part] = total.astype(BF16)

        @pl.when(me != last)
        def _():
            sum_copy(way, c).start()

        @pl.when(me == last)
        def _():
            total = own[c, part].astype(F32) + incoming[c].astype(F32)
            scale = inv[:, 0:1]
            gate = total[:, :CF] * scale
            up = total[:, CF:] * scale
            hid[c, part * half : (part + 1) * half, :] = (
                gate / (1.0 + jnp.exp(-gate)) * up
            ).astype(BF16)
            hid_copy(part, c).start()

    def hid_stage(way, c):
        first = 0 if way == 0 else E
        last = E - first

        @pl.when(me != first)
        def _():
            hid_copy(way, c).wait_recv()

            @pl.when(me != last)
            def _():
                hid_copy(way, c).start()

    def inside(c):
        return jnp.logical_and(c >= 0, c < NC)

    acc[...] = jnp.zeros_like(acc)

    @pl.loop(0, NC + 2 * E)
    def _(i):
        @pl.when(i < NC)
        def _():
            ffn_copy(0, i).wait()
            gate = jnp.dot(x_all[...], wg[i], preferred_element_type=F32).astype(BF16)
            own[i, 0, :, :CF] = gate[:half]
            own[i, 1, :, :CF] = gate[half:]
            ffn_copy(1, i).wait()
            up = jnp.dot(x_all[...], wu[i], preferred_element_type=F32).astype(BF16)
            own[i, 0, :, CF:] = up[:half]
            own[i, 1, :, CF:] = up[half:]

        for way in (0, 1):
            c = i - (me if way == 0 else E - me)

            @pl.when(inside(c))
            def _():
                sum_stage(way, c)

        for way in (0, 1):
            c = i - E - (me if way == 0 else E - me)

            @pl.when(inside(c))
            def _():
                hid_stage(way, c)

        c = i - E - jnp.maximum(me, E - me)

        @pl.when(inside(c))
        def _():
            ffn_copy(2, c).wait()
            for j in range(NJ):
                cols = slice(j * WC, (j + 1) * WC)
                acc[:, cols] += jnp.dot(hid[c], wd[c, :, cols], preferred_element_type=F32)

    for j in range(NJ):
        cols = slice(j * WC, (j + 1) * WC)
        down[:, cols] = acc[:, cols].astype(BF16)
        for k in range(1, nc):
            rs_copy(k, j, down, down_in, dn_s, dn_r).start()
    for j in range(NJ):
        cols = slice(j * WC, (j + 1) * WC)
        value = stream[:, cols] + acc[my_rows, cols]
        for k in range(1, nc):
            rs_copy(k, j, down, down_in, dn_s, dn_r).wait_recv()
            value = value + down_in[k - 1, :, cols].astype(F32)
        out_ref[:, cols] = value.astype(BF16)

    for k in range(1, nc):
        for j in range(NJ):
            rs_copy(k, j, proj, rs_in, rs_s, rs_r).wait_send()
            x_copy(k, j).wait_send()
            rs_copy(k, j, down, down_in, dn_s, dn_r).wait_send()
        ssc_copy(k).wait_send()

    for a in range(NA):
        @pl.loop(0, nd)
        def _(origin):
            @pl.when(jnp.logical_and(me < E, origin <= me))
            def _():
                att_copy(origin, a, 0, False).wait_send()

            @pl.when(jnp.logical_and(me > 0, origin >= me))
            def _():
                att_copy(origin, a, 1, False).wait_send()

    for way in (0, 1):
        @pl.when(me != (E if way == 0 else 0))
        def _():
            ssd_copy(way).wait_send()

            @pl.loop(0, NC)
            def _(c):
                sum_copy(way, c).wait_send()
                hid_copy(way, c).wait_send()


def layer(nd, nc, attended, seats, resid, gain, w_out, w_gate, w_up, w_down):
    B, HK = attended.shape
    T = seats.shape[1]
    R, DK = resid.shape
    FK = w_gate.shape[1]
    WC = divisor(DK, (512, 256, 128))
    NJ = DK // WC
    AC = divisor(HK, (1024, 512, 256, 128))
    NA = HK // AC
    CF = divisor(FK, (512, 256, 128))
    NC = FK // CF
    half = T // 2
    dims = (T, B, R, HK, WC, NJ, AC, NA, CF, NC, half, float(DK * nd))
    dma = pltpu.SemaphoreType.DMA
    vmem = pl.BlockSpec(memory_space=pltpu.VMEM)
    hbm = pl.BlockSpec(memory_space=pltpu.HBM)
    scratch = [
        pltpu.VMEM((NJ, HK, WC), BF16),
        pltpu.VMEM((NC, DK, CF), BF16),
        pltpu.VMEM((NC, DK, CF), BF16),
        pltpu.VMEM((NC, CF, DK), BF16),
        pltpu.VMEM((T, HK), BF16),
        pltpu.VMEM((T, HK), BF16),
        pltpu.VMEM((T, DK), BF16),
        pltpu.VMEM((nc - 1, R, DK), BF16),
        pltpu.VMEM((T, DK), BF16),
        pltpu.VMEM((T, 128), F32),
        pltpu.VMEM((R, DK), F32),
        pltpu.VMEM((NC, 2, half, 2 * CF), BF16),
        pltpu.VMEM((NC, half, 2 * CF), BF16),
        pltpu.VMEM((NC, half, 2 * CF), BF16),
        pltpu.VMEM((T, 128), F32),
        pltpu.VMEM((half, 128), F32),
        pltpu.VMEM((half, 128), F32),
        pltpu.VMEM((half, 128), F32),
        pltpu.VMEM((NC, T, CF), BF16),
        pltpu.VMEM((T, DK), F32),
        pltpu.VMEM((T, DK), BF16),
        pltpu.VMEM((nc - 1, R, DK), BF16),
        dma((NJ,)),
        dma((3, NC)),
        dma((2, nd, NA)),
        dma((nd, NA)),
        dma((nc - 1, NJ)),
        dma((nc - 1, NJ)),
        dma((nc - 1, NJ)),
        dma((nc - 1, NJ)),
        dma((nc - 1,)),
        dma((nc - 1,)),
        dma((2, NC)),
        dma((2, NC)),
        dma((2,)),
        dma((2,)),
        dma((2, NC)),
        dma((2, NC)),
        dma((nc - 1, NJ)),
        dma((nc - 1, NJ)),
    ]
    return pl.pallas_call(
        functools.partial(layer_kernel, nd, nc, dims),
        out_shape=jax.ShapeDtypeStruct((R, DK), BF16),
        in_specs=[vmem] * 4 + [hbm] * 4,
        out_specs=vmem,
        scratch_shapes=scratch,
        compiler_params=pltpu.CompilerParams(
            collective_id=0, has_side_effects=True, vmem_limit_bytes=67043328
        ),
    )(attended, seats, resid, gain, w_out, w_gate, w_up, w_down)


def solution(mesh):
    nd, nc = mesh.shape["dev"], mesh.shape["col"]

    def on_device(
        queries,
        kv_pages,
        page_table,
        seq_lengths,
        ffn_seat,
        resid,
        w_out,
        norm_gain,
        w_gate,
        w_up,
        w_down,
    ):
        attended = attend(queries, kv_pages, page_table, seq_lengths)
        return layer(
            nd, nc, attended, ffn_seat[None, :], resid, norm_gain[None, :], w_out, w_gate, w_up, w_down
        )

    in_specs = (
        P(("rep", "dev"), "col"),
        P(("rep", "dev"), "col", None, None, None),
        P(("rep", "dev"), None),
        P(("rep", "dev")),
        P("rep"),
        P(("rep", "col"), "dev"),
        P("col", "dev"),
        P("dev"),
        P("dev", "col"),
        P("dev", "col"),
        P("col", "dev"),
    )
    return jax.shard_map(
        on_device,
        mesh=mesh,
        in_specs=in_specs,
        out_specs=P(("rep", "col"), "dev"),
        check_vma=False,
    )
```
